128 devices in a mesh: dp: 1, sp: 128 (over z, y, x, core).
Axes of the slice: x: 4, y: 4, z: 4, core: 2. Of those that a mesh axis runs over, the one named last changes fastest.
Arguments:
- tokens: bfloat16 [32768, 2048], P(('dp', 'sp'))
- w_q: bfloat16 [2048, 32, 64], replicated
- w_k: bfloat16 [2048, 32, 64], replicated
- w_v: bfloat16 [2048, 32, 64], replicated
- w_o: bfloat16 [2048, 32, 64], replicated
- rand_idx: int32 [512, 12], P(('dp', 'sp'))
Outputs:
- output: bfloat16 [32768, 2048], P(('dp', 'sp'))
All inputs are finite; a program needn't handle non-finite values.
Results may differ from the reference program's by a relative error of at most 0.00323.
Values are sent between devices in bfloat16 or wider.
A program may use at most 1 GiB of HBM per device.

```python
import jax
import jax.numpy as jnp
from jax import lax

D_MODEL = 2048
HEADS = 32
HEAD_DIM = 64
BLOCK = 64
RAND_BLOCKS = 12
GLOB_BLOCKS = 2
BLOCKS_DEV = 4
SEQ_DEVS = 128

NUM_BLOCKS = SEQ_DEVS * BLOCKS_DEV
SEQ_LEN = NUM_BLOCKS * BLOCK
NUM_KEYS = GLOB_BLOCKS + 2 + RAND_BLOCKS


def draw_index(key):
    key_pick, key_rank = jax.random.split(key)
    src_dev = jnp.arange(SEQ_DEVS)
    low_off = jnp.maximum(GLOB_BLOCKS - src_dev * BLOCKS_DEV, 0)
    span_len = jnp.maximum(BLOCKS_DEV - low_off, 1)
    draws = jax.random.randint(key_pick, (SEQ_DEVS, SEQ_DEVS), 0, 2 ** 20)
    chosen = src_dev[None, :] * BLOCKS_DEV + low_off[None, :] + draws % span_len[None, :]
    blk_ids = jnp.arange(NUM_BLOCKS)
    owner = blk_ids // BLOCKS_DEV
    chosen_rows = chosen[owner][:, owner]
    local = owner[:, None] == owner[None, :]
    allowed = (blk_ids[None, :] >= GLOB_BLOCKS) & (blk_ids[None, :] <= blk_ids[:, None] - 2) & (local | (chosen_rows == blk_ids[None, :]))
    noise = jax.random.randint(key_rank, (NUM_BLOCKS, NUM_BLOCKS), 0, 2 ** 19)
    score = jnp.where(allowed, (noise + jnp.where(local, 0, 2 ** 19)) * NUM_BLOCKS + blk_ids[None, :], -1 - blk_ids[None, :])
    top_val, top_pos = lax.top_k(score, RAND_BLOCKS)
    return jnp.where(top_val >= 0, top_pos, -1).astype(jnp.int32)


def setup_inputs(seed: int = 0, part: int = 0) -> dict:
    part_key = jax.random.fold_in(jax.random.key(seed), part)
    key_tok, key_idx = jax.random.split(part_key)
    key_q, key_k, key_v, key_o = jax.random.split(jax.random.key(seed + 1), 4)
    width = HEADS * HEAD_DIM
    in_scale = D_MODEL ** -0.5
    out_scale = 0.5 * (BLOCK * NUM_KEYS / width) ** 0.5
    w_shape = (D_MODEL, HEADS, HEAD_DIM)
    tokens = jax.random.normal(key_tok, (SEQ_LEN, D_MODEL), jnp.float32)
    return {
        "tokens": tokens.astype(jnp.bfloat16),
        "w_q": (jax.random.normal(key_q, w_shape, jnp.float32) * in_scale).astype(jnp.bfloat16),
        "w_k": (jax.random.normal(key_k, w_shape, jnp.float32) * in_scale).astype(jnp.bfloat16),
        "w_v": (jax.random.normal(key_v, w_shape, jnp.float32) * in_scale).astype(jnp.bfloat16),
        "w_o": (jax.random.normal(key_o, w_shape, jnp.float32) * out_scale).astype(jnp.bfloat16),
        "rand_idx": draw_index(key_idx),
    }


def reference(tokens, w_q, w_k, w_v, w_o, rand_idx):
    width = HEADS * HEAD_DIM

    def project(weight):
        proj = jnp.dot(tokens, weight.reshape(D_MODEL, width), preferred_element_type=jnp.float32)
        return proj.astype(jnp.bfloat16).reshape(NUM_BLOCKS, BLOCK, HEADS, HEAD_DIM)

    q_blocks = project(w_q)
    k_blocks = project(w_k)
    v_blocks = project(w_v)
    offsets = jnp.arange(BLOCK)
    causal = offsets[:, None] >= offsets[None, :]
    glob_ids = jnp.arange(GLOB_BLOCKS)
    is_self = jnp.arange(NUM_KEYS) == GLOB_BLOCKS + 1
    scale = HEAD_DIM ** -0.5

    def one_block(item):
        row, rand_row = item
        key_ids = jnp.concatenate([glob_ids, jnp.stack([jnp.maximum(row - 1, 0), row]), jnp.maximum(rand_row, 0)])
        valid = jnp.concatenate([glob_ids < row, jnp.stack([row - 1 >= GLOB_BLOCKS, row >= 0]), rand_row >= 0])
        keys = k_blocks[key_ids].astype(jnp.float32)
        values = v_blocks[key_ids].astype(jnp.float32)
        query = q_blocks[row].astype(jnp.float32)
        scores = jnp.einsum("qhe,kthe->hqkt", query, keys) * scale
        mask = valid[None, :, None] & (~is_self[None, :, None] | causal[:, None, :])
        scores = jnp.where(mask[None], scores, -jnp.inf)
        peak = jnp.max(scores, axis=(2, 3), keepdims=True)
        unnorm = jnp.exp(scores - peak)
        prob_bf = (unnorm / jnp.sum(unnorm, axis=(2, 3), keepdims=True)).astype(jnp.bfloat16)
        context = jnp.einsum("hqkt,kthe->qhe", prob_bf.astype(jnp.float32), values)
        return context.astype(jnp.bfloat16)

    ctx_all = lax.map(one_block, (jnp.arange(NUM_BLOCKS), rand_idx))
    ctx_flat = ctx_all.reshape(SEQ_LEN, width)
    result = jnp.dot(ctx_flat, w_o.reshape(D_MODEL, width).T, preferred_element_type=jnp.float32)
    return result.astype(jnp.bfloat16)
```

```python
import functools

import jax
import jax.numpy as jnp
from jax import lax
from jax.experimental import pallas as pl
from jax.experimental.pallas import tpu as pltpu
from jax.sharding import PartitionSpec as P

GLOB_BLOCKS = 2
HEAD_GROUP = 4
TILE_BLOCKS = 8
COLS = 256
LOG2E = 1.4426950408889634


def attend_kernel(
    proj_steps, blocks_dev, num_keys, block, head_dim,
    ids_ref, count_ref, slots_ref,
    q_ref, bias_ref, tok_ref, wk_ref, wv_ref, wo_ref, kn_ref, vn_ref,
    out_ref,
    kpool, vpool, xbuf, wbuf, ctx,
    x_sem, w_sem, near_sem,
):
    step = pl.program_id(0)
    used = count_ref[0]
    far = proj_steps * TILE_BLOCKS
    width = q_ref.shape[1]

    def x_copy(at, g):
        return pltpu.make_async_copy(tok_ref.at[ids_ref[at * TILE_BLOCKS + g]], xbuf.at[lax.rem(at, 2), g], x_sem.at[lax.rem(at, 2), g])

    def w_copy(src, which):
        return pltpu.make_async_copy(src, wbuf.at[which], w_sem.at[which])

    def near_copies():
        return (
            pltpu.make_async_copy(kn_ref, kpool.at[pl.ds(far, blocks_dev)], near_sem.at[0]),
            pltpu.make_async_copy(vn_ref, vpool.at[pl.ds(far, blocks_dev)], near_sem.at[1]),
        )

    @pl.when(step == 0)
    def _():
        for g in range(TILE_BLOCKS):
            x_copy(0, g).start()
        w_copy(wk_ref, 0).start()
        w_copy(wv_ref, 1).start()
        for copy in near_copies():
            copy.start()

    @pl.when(step + 1 < used)
    def _():
        for g in range(TILE_BLOCKS):
            x_copy(step + 1, g).start()

    def fill(pool, which):
        def column(c, carry):
            at = pl.ds(pl.multiple_of(c * COLS, COLS), COLS)
            tok = xbuf[lax.rem(step, 2)].reshape(TILE_BLOCKS * block, -1)
            proj = jnp.dot(tok, wbuf[which, :, at], preferred_element_type=jnp.float32)
            pool[pl.ds(step * TILE_BLOCKS, TILE_BLOCKS), :, at] = proj.astype(jnp.bfloat16).reshape(TILE_BLOCKS, block, COLS)
            return carry

        lax.fori_loop(0, width // COLS, column, 0)

    @pl.when(step < used)
    def _():
        for g in range(TILE_BLOCKS):
            x_copy(step, g).wait()

        @pl.when(step == 0)
        def _():
            w_copy(wk_ref, 0).wait()

        fill(kpool, 0)

        @pl.when(step == 0)
        def _():
            w_copy(wv_ref, 1).wait()

        fill(vpool, 1)

    @pl.when(step == proj_steps)
    def _():
        w_copy(wo_ref, 0).start()
        for copy in near_copies():
            copy.wait()

    @pl.when(step >= proj_steps)
    def _():
        row = step - proj_steps
        wide = HEAD_GROUP * head_dim
        rows = HEAD_GROUP * block
        keys = num_keys * block
        factor = head_dim ** -0.5 * LOG2E
        lane_head = lax.broadcasted_iota(jnp.int32, (block, wide), 1) // head_dim
        q_pos = lax.rem(lax.broadcasted_iota(jnp.int32, (rows, 2 * block), 0), block)
        k_pos = lax.broadcasted_iota(jnp.int32, (rows, 2 * block), 1)
        causal = (k_pos <= q_pos) | (k_pos >= block)
        bias = bias_ref[0]
        slots = [slots_ref[row * num_keys + j] for j in range(num_keys)]

        def heads(g, carry):
            lanes = pl.ds(pl.multiple_of(g * wide, wide), wide)
            q = q_ref[:, lanes]
            zero = jnp.zeros_like(q)
            q_diag = jnp.concatenate([jnp.where(lane_head == h, q, zero) for h in range(HEAD_GROUP)], axis=0)
            k = jnp.concatenate([kpool[slot, :, lanes] for slot in slots], axis=0)
            scores = lax.dot_general(q_diag, k, (((1,), (1,)), ((), ())), preferred_element_type=jnp.float32) + bias
            own = jnp.where(causal, scores[:, : 2 * block], -jnp.inf)
            scores = jnp.concatenate([own, scores[:, 2 * block :]], axis=1)
            peak = jnp.max(scores, axis=1, keepdims=True)
            unnorm = jnp.exp2((scores - peak) * factor)
            total = jnp.sum(unnorm, axis=1, keepdims=True)
            prob = (unnorm * (1.0 / total)).astype(jnp.bfloat16)
            v = jnp.concatenate([vpool[slot, :, lanes] for slot in slots], axis=0)
            mixed = jnp.dot(prob, v, preferred_element_type=jnp.float32)
            picked = mixed[:block]
            for h in range(1, HEAD_GROUP):
                picked = jnp.where(lane_head == h, mixed[h * block : (h + 1) * block], picked)
            ctx[pl.ds(pl.multiple_of(row * block, block), block), lanes] = picked.astype(jnp.bfloat16)
            return carry

        lax.fori_loop(0, width // wide, heads, 0)

    @pl.when(step == proj_steps + blocks_dev - 1)
    def _():
        w_copy(wo_ref, 0).wait()

        def column(c, carry):
            at = pl.ds(pl.multiple_of(c * COLS, COLS), COLS)
            out_ref[:, at] = jnp.dot(ctx[...], wbuf[0, :, at], preferred_element_type=jnp.float32).astype(jnp.bfloat16)
            return carry

        lax.fori_loop(0, out_ref.shape[1] // COLS, column, 0)


def attend(ids, count, slots, q, bias, tok, wk, wv, wo, k_near, v_near, head_dim):
    blocks_dev, block, width = k_near.shape
    model = wo.shape[1]
    proj_steps = ids.shape[0] // TILE_BLOCKS
    num_keys = slots.shape[0] // blocks_dev
    pool = proj_steps * TILE_BLOCKS + blocks_dev
    any_spec = pl.BlockSpec(memory_space=pl.ANY)
    row_of = lambda i: jnp.maximum(i - proj_steps, 0)
    grid_spec = pltpu.PrefetchScalarGridSpec(
        num_scalar_prefetch=3,
        grid=(proj_steps + blocks_dev,),
        in_specs=[
            pl.BlockSpec((block, width), lambda i, *_: (row_of(i), 0)),
            pl.BlockSpec((1, 1, num_keys * block), lambda i, *_: (row_of(i), 0, 0)),
        ] + [any_spec] * 6,
        out_specs=pl.BlockSpec((blocks_dev * block, model), lambda i, *_: (0, 0)),
        scratch_shapes=[
            pltpu.VMEM((pool, block, width), jnp.bfloat16),
            pltpu.VMEM((pool, block, width), jnp.bfloat16),
            pltpu.VMEM((2, TILE_BLOCKS, block, model), jnp.bfloat16),
            pltpu.VMEM((2, model, width), jnp.bfloat16),
            pltpu.VMEM((blocks_dev * block, width), jnp.bfloat16),
            pltpu.SemaphoreType.DMA((2, TILE_BLOCKS)),
            pltpu.SemaphoreType.DMA((2,)),
            pltpu.SemaphoreType.DMA((2,)),
        ],
    )
    return pl.pallas_call(
        functools.partial(attend_kernel, proj_steps, blocks_dev, num_keys, block, head_dim),
        grid_spec=grid_spec,
        out_shape=jax.ShapeDtypeStruct((blocks_dev * block, model), jnp.bfloat16),
        compiler_params=pltpu.CompilerParams(dimension_semantics=("arbitrary",), vmem_limit_bytes=67043328),
        cost_estimate=pl.CostEstimate(flops=70_000_000_000, bytes_accessed=60_000_000, transcendentals=8_000_000),
        name="attend",
    )(ids, count, slots, q, bias, tok, wk, wv, wo, k_near, v_near)


def solution(mesh):
    seq_devs = mesh.shape["sp"]
    row_spec = P(("dp", "sp"), None)
    weight_spec = P(None, None, None)

    def local_fn(tokens, w_q, w_k, w_v, w_o, rand_idx):
        me = lax.axis_index("sp")
        blocks_dev, rand_count = rand_idx.shape
        block = tokens.shape[0] // blocks_dev
        model, heads, head_dim = w_q.shape
        width = heads * head_dim
        all_tok = lax.all_gather(tokens, "sp", axis=0, tiled=True).reshape(seq_devs * blocks_dev, block, model)

        wq, wk, wv = (w.reshape(model, width) for w in (w_q, w_k, w_v))
        wo = jnp.transpose(w_o, (1, 2, 0)).reshape(width, model)

        def project(weight):
            return jnp.dot(tokens, weight, preferred_element_type=jnp.float32).astype(jnp.bfloat16)

        q_loc = project(wq)
        k_near = project(wk).reshape(blocks_dev, block, width)
        v_near = project(wv).reshape(blocks_dev, block, width)

        first_row = me * blocks_dev
        local = jnp.arange(blocks_dev)
        rows = first_row + local
        devs = jnp.arange(seq_devs)
        owner = rand_idx // blocks_dev
        hits = (owner[:, :, None] == devs) & (rand_idx[:, :, None] >= 0)
        wanted = jnp.max(jnp.where(hits, rand_idx[:, :, None], -1), axis=(0, 1))
        need = ((wanted >= 0) & (devs != me)).astype(jnp.int32)
        fixed = GLOB_BLOCKS + 1
        slot_of = fixed + jnp.cumsum(need) - need
        steps = -(-(fixed + blocks_dev * rand_count) // TILE_BLOCKS)
        pool_rows = steps * TILE_BLOCKS
        total = fixed + jnp.sum(need)
        used = (total + TILE_BLOCKS - 1) // TILE_BLOCKS
        place = jnp.arange(pool_rows)
        ids = jnp.sum(jnp.where((slot_of[None, :] == place[:, None]) & (need[None, :] > 0), wanted[None, :], 0), axis=1)
        ids = ids + jnp.where(place < GLOB_BLOCKS, place, jnp.where(place == GLOB_BLOCKS, jnp.maximum(first_row - 1, 0), 0))
        far_pos = jnp.sum(jnp.where(hits, slot_of, 0), axis=2)
        rand_pos = jnp.where(rand_idx < 0, pool_rows, jnp.where(owner == me, pool_rows + rand_idx - first_row, far_pos))
        prev = jnp.where(local == 0, GLOB_BLOCKS, pool_rows + local - 1)
        lead = jnp.broadcast_to(jnp.arange(GLOB_BLOCKS), (blocks_dev, GLOB_BLOCKS))
        slots = jnp.concatenate([pool_rows + local[:, None], prev[:, None], lead, rand_pos], axis=1).reshape(-1)
        valid = jnp.concatenate([jnp.ones((blocks_dev, 1), jnp.bool_), (rows - 1 >= GLOB_BLOCKS)[:, None], jnp.arange(GLOB_BLOCKS)[None, :] < rows[:, None], rand_idx >= 0], axis=1)
        bias = jnp.where(jnp.repeat(valid, block, axis=1), 0.0, -jnp.inf).astype(jnp.float32)[:, None, :]
        i32 = lambda a: a.astype(jnp.int32)
        return attend(i32(ids), i32(used)[None], i32(slots), q_loc, bias, all_tok, wk, wv, wo, k_near, v_near, head_dim)

    return jax.shard_map(local_fn, mesh=mesh, in_specs=(row_spec, weight_spec, weight_spec, weight_spec, weight_spec, row_spec), out_specs=row_spec, check_vma=False)
```

```python
import functools

import jax
import jax.numpy as jnp
from jax import lax
from jax.experimental import pallas as pl
from jax.experimental.pallas import tpu as pltpu
from jax.sharding import PartitionSpec as P

GLOB_BLOCKS = 2
HEAD_GROUP = 4
TILE_BLOCKS = 8
COLS = 1024
LOG2E = 1.4426950408889634


def attend_kernel(
    proj_steps, blocks_dev, num_keys, block, head_dim,
    ids_ref, count_ref, slots_ref,
    q_ref, bias_ref, tok_ref, wk_ref, wv_ref, wo_ref, kn_ref, vn_ref,
    out_ref,
    kpool, vpool, xbuf, wbuf, ctx,
    x_sem, w_sem, near_sem,
):
    step = pl.program_id(0)
    used = count_ref[0]
    far = proj_steps * TILE_BLOCKS
    width = q_ref.shape[1]

    def x_copy(at, g):
        return pltpu.make_async_copy(tok_ref.at[ids_ref[at * TILE_BLOCKS + g]], xbuf.at[lax.rem(at, 2), g], x_sem.at[lax.rem(at, 2), g])

    def w_copy(src, which, c):
        return pltpu.make_async_copy(src.at[:, pl.ds(c * COLS, COLS)], wbuf.at[which, :, pl.ds(c * COLS, COLS)], w_sem.at[which, c])

    def near_copies():
        return (
            pltpu.make_async_copy(kn_ref, kpool.at[pl.ds(far, blocks_dev)], near_sem.at[0]),
            pltpu.make_async_copy(vn_ref, vpool.at[pl.ds(far, blocks_dev)], near_sem.at[1]),
        )

    @pl.when(step == 0)
    def _():
        for g in range(TILE_BLOCKS):
            x_copy(0, g).start()
        for c in range(width // COLS):
            w_copy(wk_ref, 0, c).start()
        for c in range(width // COLS):
            w_copy(wv_ref, 1, c).start()
        for copy in near_copies():
            copy.start()

    @pl.when(step + 1 < used)
    def _():
        for g in range(TILE_BLOCKS):
            x_copy(step + 1, g).start()

    def fill(pool, weight, which):
        def column(c, carry):
            @pl.when(step == 0)
            def _():
                w_copy(weight, which, c).wait()

            at = pl.ds(pl.multiple_of(c * COLS, COLS), COLS)
            tok = xbuf[lax.rem(step, 2)].reshape(TILE_BLOCKS * block, -1)
            proj = jnp.dot(tok, wbuf[which, :, at], preferred_element_type=jnp.float32)
            pool[pl.ds(step * TILE_BLOCKS, TILE_BLOCKS), :, at] = proj.astype(jnp.bfloat16).reshape(TILE_BLOCKS, block, COLS)
            return carry

        lax.fori_loop(0, width // COLS, column, 0)

    @pl.when(step < used)
    def _():
        for g in range(TILE_BLOCKS):
            x_copy(step, g).wait()

        fill(kpool, wk_ref, 0)
        fill(vpool, wv_ref, 1)

    @pl.when(step == proj_steps)
    def _():
        for c in range(width // COLS):
            w_copy(wo_ref, 0, c).start()
        for copy in near_copies():
            copy.wait()

    @pl.when(step >= proj_steps)
    def _():
        row = step - proj_steps
        wide = HEAD_GROUP * head_dim
        rows = HEAD_GROUP * block
        keys = num_keys * block
        factor = head_dim ** -0.5 * LOG2E
        lane_head = lax.broadcasted_iota(jnp.int32, (block, wide), 1) // head_dim
        q_pos = lax.rem(lax.broadcasted_iota(jnp.int32, (rows, 2 * block), 0), block)
        k_pos = lax.broadcasted_iota(jnp.int32, (rows, 2 * block), 1)
        causal = (k_pos <= q_pos) | (k_pos >= block)
        bias = bias_ref[0]
        slots = [slots_ref[row * num_keys + j] for j in range(num_keys)]

        def heads(g, carry):
            lanes = pl.ds(pl.multiple_of(g * wide, wide), wide)
            q = q_ref[:, lanes]
            zero = jnp.zeros_like(q)
            q_diag = jnp.concatenate([jnp.where(lane_head == h, q, zero) for h in range(HEAD_GROUP)], axis=0)
            k = jnp.concatenate([kpool[slot, :, lanes] for slot in slots], axis=0)
            scores = lax.dot_general(q_diag, k, (((1,), (1,)), ((), ())), preferred_element_type=jnp.float32) + bias
            own = jnp.where(causal, scores[:, : 2 * block], -jnp.inf)
            scores = jnp.concatenate([own, scores[:, 2 * block :]], axis=1)
            peak = jnp.max(scores, axis=1, keepdims=True)
            unnorm = jnp.exp2((scores - peak) * factor)
            total = jnp.sum(unnorm, axis=1, keepdims=True)
            prob = (unnorm * (1.0 / total)).astype(jnp.bfloat16)
            v = jnp.concatenate([vpool[slot, :, lanes] for slot in slots], axis=0)
            mixed = jnp.dot(prob, v, preferred_element_type=jnp.float32)
            picked = mixed[:block]
            for h in range(1, HEAD_GROUP):
                picked = jnp.where(lane_head == h, mixed[h * block : (h + 1) * block], picked)
            ctx[pl.ds(pl.multiple_of(row * block, block), block), lanes] = picked.astype(jnp.bfloat16)
            return carry

        lax.fori_loop(0, width // wide, heads, 0, unroll=8)

    @pl.when(step == proj_steps + blocks_dev - 1)
    def _():
        def column(c, carry):
            w_copy(wo_ref, 0, c).wait()
            at = pl.ds(pl.multiple_of(c * COLS, COLS), COLS)
            out_ref[:, at] = jnp.dot(ctx[...], wbuf[0, :, at], preferred_element_type=jnp.float32).astype(jnp.bfloat16)
            return carry

        lax.fori_loop(0, out_ref.shape[1] // COLS, column, 0)


def attend(ids, count, slots, q, bias, tok, wk, wv, wo, k_near, v_near, head_dim):
    blocks_dev, block, width = k_near.shape
    model = wo.shape[1]
    proj_steps = ids.shape[0] // TILE_BLOCKS
    num_keys = slots.shape[0] // blocks_dev
    pool = proj_steps * TILE_BLOCKS + blocks_dev
    any_spec = pl.BlockSpec(memory_space=pl.ANY)
    row_of = lambda i: jnp.maximum(i - proj_steps, 0)
    grid_spec = pltpu.PrefetchScalarGridSpec(
        num_scalar_prefetch=3,
        grid=(proj_steps + blocks_dev,),
        in_specs=[
            pl.BlockSpec((block, width), lambda i, *_: (row_of(i), 0)),
            pl.BlockSpec((1, 1, num_keys * block), lambda i, *_: (row_of(i), 0, 0)),
        ] + [any_spec] * 6,
        out_specs=pl.BlockSpec((blocks_dev * block, model), lambda i, *_: (0, 0)),
        scratch_shapes=[
            pltpu.VMEM((pool, block, width), jnp.bfloat16),
            pltpu.VMEM((pool, block, width), jnp.bfloat16),
            pltpu.VMEM((2, TILE_BLOCKS, block, model), jnp.bfloat16),
            pltpu.VMEM((2, model, width), jnp.bfloat16),
            pltpu.VMEM((blocks_dev * block, width), jnp.bfloat16),
            pltpu.SemaphoreType.DMA((2, TILE_BLOCKS)),
            pltpu.SemaphoreType.DMA((2, width // COLS)),
            pltpu.SemaphoreType.DMA((2,)),
        ],
    )
    return pl.pallas_call(
        functools.partial(attend_kernel, proj_steps, blocks_dev, num_keys, block, head_dim),
        grid_spec=grid_spec,
        out_shape=jax.ShapeDtypeStruct((blocks_dev * block, model), jnp.bfloat16),
        compiler_params=pltpu.CompilerParams(dimension_semantics=("arbitrary",), vmem_limit_bytes=67043328),
        cost_estimate=pl.CostEstimate(flops=70_000_000_000, bytes_accessed=60_000_000, transcendentals=8_000_000),
        name="attend",
    )(ids, count, slots, q, bias, tok, wk, wv, wo, k_near, v_near)


def solution(mesh):
    seq_devs = mesh.shape["sp"]
    row_spec = P(("dp", "sp"), None)
    weight_spec = P(None, None, None)

    def local_fn(tokens, w_q, w_k, w_v, w_o, rand_idx):
        me = lax.axis_index("sp")
        blocks_dev, rand_count = rand_idx.shape
        block = tokens.shape[0] // blocks_dev
        model, heads, head_dim = w_q.shape
        width = heads * head_dim
        all_tok = lax.all_gather(tokens, "sp", axis=0, tiled=True).reshape(seq_devs * blocks_dev, block, model)

        wq, wk, wv = (w.reshape(model, width) for w in (w_q, w_k, w_v))
        wo = jnp.transpose(w_o, (1, 2, 0)).reshape(width, model)

        def project(weight):
            return jnp.dot(tokens, weight, preferred_element_type=jnp.float32).astype(jnp.bfloat16)

        q_loc = project(wq)
        k_near = project(wk).reshape(blocks_dev, block, width)
        v_near = project(wv).reshape(blocks_dev, block, width)

        first_row = me * blocks_dev
        local = jnp.arange(blocks_dev)
        rows = first_row + local
        devs = jnp.arange(seq_devs)
        owner = rand_idx // blocks_dev
        hits = (owner[:, :, None] == devs) & (rand_idx[:, :, None] >= 0)
        wanted = jnp.max(jnp.where(hits, rand_idx[:, :, None], -1), axis=(0, 1))
        need = ((wanted >= 0) & (devs != me)).astype(jnp.int32)
        fixed = GLOB_BLOCKS + 1
        slot_of = fixed + jnp.cumsum(need) - need
        steps = -(-(fixed + blocks_dev * rand_count) // TILE_BLOCKS)
        pool_rows = steps * TILE_BLOCKS
        total = fixed + jnp.sum(need)
        used = (total + TILE_BLOCKS - 1) // TILE_BLOCKS
        place = jnp.arange(pool_rows)
        ids = jnp.sum(jnp.where((slot_of[None, :] == place[:, None]) & (need[None, :] > 0), wanted[None, :], 0), axis=1)
        ids = ids + jnp.where(place < GLOB_BLOCKS, place, jnp.where(place == GLOB_BLOCKS, jnp.maximum(first_row - 1, 0), 0))
        far_pos = jnp.sum(jnp.where(hits, slot_of, 0), axis=2)
        rand_pos = jnp.where(rand_idx < 0, pool_rows, jnp.where(owner == me, pool_rows + rand_idx - first_row, far_pos))
        prev = jnp.where(local == 0, GLOB_BLOCKS, pool_rows + local - 1)
        lead = jnp.broadcast_to(jnp.arange(GLOB_BLOCKS), (blocks_dev, GLOB_BLOCKS))
        slots = jnp.concatenate([pool_rows + local[:, None], prev[:, None], lead, rand_pos], axis=1).reshape(-1)
        valid = jnp.concatenate([jnp.ones((blocks_dev, 1), jnp.bool_), (rows - 1 >= GLOB_BLOCKS)[:, None], jnp.arange(GLOB_BLOCKS)[None, :] < rows[:, None], rand_idx >= 0], axis=1)
        bias = jnp.where(jnp.repeat(valid, block, axis=1), 0.0, -jnp.inf).astype(jnp.float32)[:, None, :]
        i32 = lambda a: a.astype(jnp.int32)
        return attend(i32(ids), i32(used)[None], i32(slots), q_loc, bias, all_tok, wk, wv, wo, k_near, v_near, head_dim)

    return jax.shard_map(local_fn, mesh=mesh, in_specs=(row_spec, weight_spec, weight_spec, weight_spec, weight_spec, row_spec), out_specs=row_spec, check_vma=False)
```
